768 devices in a mesh: az: 12 (over z_lo, x), rad: 64 (over y, z_hi, core).
Axes of the slice: x: 4, y: 8, z: 12 (z_hi: 4, z_lo: 3; z = z_hi * 3 + z_lo), core: 2. Of those that a mesh axis runs over, the one named last changes fastest.
Arguments:
- fields: float32 [5, 768, 32, 1536], P(None, 'rad', None, 'az'), may hold values from -6 to 6
- shift: int32 [768], replicated, may hold values from 0 to 1535
- fraction: float32 [768], replicated, may hold values from -0.5 to 0.5
- radial_rate: float32 [768, 32], replicated, may hold values from -0.4 to 0.4
Outputs:
- updated: float32 [5, 768, 32, 1536], P(None, 'rad', None, 'az')
The draws below stay inside these ranges and needn't reach their ends.
All inputs are finite; a program needn't handle non-finite values.
Results may differ from the reference program's by a relative error of at most 0.0003.
Values sent between devices are 32-bit elements; how exact they have to be, the bound alone decides.
A program may use at most 64 MiB of HBM per device.

```python
import jax
import jax.numpy as jnp
from jax import lax

NP = 32
NF = 5
NA = 1536
NR = 768


def touch_ends(entries, rng, low, largest):
    extent = entries.shape
    index_at = [jax.random.randint(jax.random.fold_in(rng, axis), (), 0, extent[axis]) for axis in range(len(extent))]
    entries = entries.at[tuple(index_at)].set(low)
    longest = extent.index(max(extent))
    index_at[longest] = (index_at[longest] + 1) % extent[longest]
    return entries.at[tuple(index_at)].set(largest)


def level_of(key, shape, cuts, low, high):
    level, own = 1.0, jax.random.fold_in(key, 6)
    for dim, shards_of in cuts:
        steps = jnp.exp(jax.random.uniform(jax.random.fold_in(own, dim), (shards_of,), jnp.float32, low / len(cuts), high / len(cuts)))
        level = level * jnp.repeat(steps, shape[dim] // shards_of).reshape([-1 if axis == dim else 1 for axis in range(len(shape))])
    return level


def gaussian(key, dims, scale, reach, pieces=(), kind=jnp.bfloat16):
    entries = scale * jax.random.normal(key, dims, jnp.float32)
    if pieces:
        entries = entries * level_of(key, dims, pieces, -0.22, 0.18)
    return jnp.clip(entries, -reach, reach).astype(kind)


def setup_inputs(seed: int = 0) -> dict:
    splits = jax.random.split(jax.random.key(seed), 5)
    fields = gaussian(splits[0], (NF, NR, NP, NA), 1.0, 6.0, ((1, 64), (3, 12)), jnp.float32)
    shift = touch_ends(jax.random.randint(splits[1], (NR,), 0, NA), jax.random.fold_in(splits[1], 1), 0, NA - 1).astype(jnp.int32)
    fraction = jnp.clip(jax.random.uniform(splits[2], (NR,), jnp.float32, -0.5, 0.5), -0.5, 0.5)
    radial_rate = jnp.clip(jax.random.uniform(splits[3], (NR, NP), jnp.float32, -0.4, 0.4), -0.4, 0.4)
    return {"fields": fields, "shift": shift, "fraction": fraction, "radial_rate": radial_rate}


def cut(values, low, count, axis):
    return lax.slice_in_dim(values, low, low + count, axis=axis)


def limited(left, right):
    steep = jnp.minimum(jnp.minimum(2.0 * jnp.abs(left), 2.0 * jnp.abs(right)), 0.5 * jnp.abs(left + right))
    return jnp.where(left * right > 0.0, jnp.sign(left) * steep, 0.0)


def flux_change(padded, courant, axis):
    count = padded.shape[axis] - 4
    left = cut(padded, 1, count + 2, axis) - cut(padded, 0, count + 2, axis)
    right = cut(padded, 2, count + 2, axis) - cut(padded, 1, count + 2, axis)
    slope = limited(left, right)
    forward = cut(padded, 1, count + 1, axis) + 0.5 * (1.0 - courant) * cut(slope, 0, count + 1, axis)
    backward = cut(padded, 2, count + 1, axis) - 0.5 * (1.0 + courant) * cut(slope, 1, count + 1, axis)
    flux = courant * jnp.where(courant > 0.0, forward, backward)
    return cut(flux, 1, count, axis) - cut(flux, 0, count, axis)


def one_field(single, shift, fraction, face_rates):
    rolled = lax.map(lambda item: jnp.roll(item[0], item[1], axis=-1), (single, shift))
    padded = jnp.concatenate([rolled[:, :, -2:], rolled, rolled[:, :, :2]], axis=2)
    azimuthal = rolled - flux_change(padded, fraction[:, None, None], 2)
    zeros = jnp.zeros((2,) + azimuthal.shape[1:], jnp.float32)
    radial = jnp.concatenate([zeros, azimuthal, zeros], axis=0)
    return azimuthal - flux_change(radial, face_rates[:, :, None], 0)


def reference(fields, shift, fraction, radial_rate):
    edge = jnp.zeros((1, radial_rate.shape[1]), jnp.float32)
    face_rates = jnp.concatenate([edge, radial_rate[:-1], edge], axis=0)
    return lax.map(lambda single: one_field(single, shift, fraction, face_rates), fields)
```

```python
import functools

import jax
import jax.numpy as jnp
from jax import lax
from jax.experimental import pallas as pl
from jax.experimental.pallas import tpu as pltpu
from jax.sharding import PartitionSpec as P

MESH = pl.DeviceIdType.MESH
LANES = 128
SUB = 8


def limited(left, right):
    steep = jnp.minimum(
        jnp.minimum(2.0 * jnp.abs(left), 2.0 * jnp.abs(right)), 0.5 * jnp.abs(left + right)
    )
    return jnp.where(left * right > 0.0, jnp.where(left > 0.0, steep, -steep), 0.0)


def blocks_back(x):
    return jnp.concatenate([x[-1:], x[:-1]], axis=0)


def blocks_on(x):
    return jnp.concatenate([x[1:], x[:1]], axis=0)


def kernel(
    n,
    groups,
    shift_ref,
    fraction_ref,
    fields_ref,
    rate_ref,
    out_ref,
    mine,
    whole,
    turned,
    rolled,
    tall,
    result,
    rate_raw,
    face_rate,
    load_sem,
    rate_sem,
    send_sem,
    gather_sem,
    row_sem,
    halo_send_sem,
    halo_sem,
    store_sem,
):
    nf, rows, polar, _ = mine.shape
    me = lax.axis_index("az")
    band = lax.axis_index("rad")
    first, last = band == 0, band == groups - 1

    for f in range(nf):
        pltpu.make_async_copy(fields_ref.at[f], mine.at[f], load_sem.at[f]).start()
    raw_rows = rate_raw.shape[0]
    low = jnp.maximum(band * rows - 1, 0) // SUB * SUB
    low = pl.multiple_of(jnp.minimum(low, groups * rows - raw_rows), SUB)
    rate_copy = pltpu.make_async_copy(rate_ref.at[pl.ds(low, raw_rows)], rate_raw, rate_sem)
    rate_copy.start()

    barrier = pltpu.get_barrier_semaphore()

    @pl.loop(1, n)
    def _(d):
        pl.semaphore_signal(
            barrier, inc=1, device_id={"az": lax.rem(me + d, n)}, device_id_type=MESH
        )

    @pl.when(jnp.logical_not(first))
    def _():
        pl.semaphore_signal(barrier, inc=1, device_id={"rad": band - 1}, device_id_type=MESH)

    @pl.when(jnp.logical_not(last))
    def _():
        pl.semaphore_signal(barrier, inc=1, device_id={"rad": band + 1}, device_id_type=MESH)

    inner = jnp.where(first, 0, 1) + jnp.where(last, 0, 1)
    pl.semaphore_wait(barrier, n - 1 + inner)

    for f in range(nf):
        pltpu.make_async_copy(fields_ref.at[f], mine.at[f], load_sem.at[f]).wait()

        @pl.loop(1, n)
        def _(d):
            to = lax.rem(me + d, n)
            pltpu.make_async_remote_copy(
                src_ref=mine.at[f, to],
                dst_ref=whole.at[f, me],
                send_sem=send_sem.at[0],
                recv_sem=gather_sem.at[f],
                device_id={"az": to},
                device_id_type=MESH,
            ).start()

    rate_copy.wait()
    at_lane = lax.broadcasted_iota(jnp.int32, (polar, polar), 1)
    at_sub = lax.broadcasted_iota(jnp.int32, (polar, polar), 0)
    for i in range(rows + 1):
        here = jnp.maximum(band * rows + i - 1, 0) - low
        line = rate_raw[pl.ds(here, 1), :]
        spread = jnp.where(at_lane == at_sub, jnp.broadcast_to(line, (polar, polar)), 0.0)
        column = jnp.sum(spread, axis=1, keepdims=True)
        if i == 0:
            column = jnp.where(first, 0.0, column)
        if i == rows:
            column = jnp.where(last, 0.0, column)
        face_rate[i] = jnp.broadcast_to(column, (polar, LANES))

    @pl.when(first)
    def _():
        tall[:, 0:2] = jnp.zeros((nf, 2, polar, LANES), jnp.float32)

    @pl.when(last)
    def _():
        tall[:, rows + 2 : rows + 4] = jnp.zeros((nf, 2, polar, LANES), jnp.float32)

    row = band * rows + me
    amount = shift_ref[row]
    courant = fraction_ref[row]
    blocks = amount >> 7
    lanes = amount & (LANES - 1)
    upwind = courant > 0.0
    weight = jnp.where(upwind, 0.5 * (1.0 - courant), -0.5 * (1.0 + courant))
    step = jnp.where(upwind, 1, LANES - 1)
    edge = jnp.where(upwind, 0, LANES - 1)
    lane = lax.broadcasted_iota(jnp.int32, (n, SUB, LANES), 2)
    lane_row = lax.broadcasted_iota(jnp.int32, (polar, LANES), 1)

    @pl.loop(0, nf)
    def _(f):
        whole[f, me] = mine[f, me]
        got = whole.at[f, pl.ds(0, n - 1)]
        pltpu.make_async_copy(got, got, gather_sem.at[f]).wait()

        for t in range(0, polar, SUB):
            q = whole[f, :, t : t + SUB, :]
            ahead = pltpu.roll(q, LANES - 1, 2)
            right = jnp.where(lane == LANES - 1, blocks_on(ahead), ahead) - q
            back = pltpu.roll(right, 1, 2)
            left = jnp.where(lane == 0, blocks_back(back), back)
            flux = courant * (q + weight * limited(left, right))
            other = pltpu.roll(flux, step, 2)
            beside = jnp.where(upwind, blocks_back(other), blocks_on(other))
            other = jnp.where(lane == edge, beside, other)
            change = jnp.where(upwind, flux - other, other - flux)
            turned[:, t : t + SUB, :] = pltpu.roll(q - change, lanes, 2)

        @pl.loop(0, n)
        def _(j):
            from_here = lax.rem(j - blocks + n, n)
            from_last = lax.rem(j - blocks - 1 + n + n, n)
            rolled[f, j] = jnp.where(lane_row >= lanes, turned[from_here], turned[from_last])

        @pl.loop(1, n)
        def _(d):
            to = lax.rem(me + d, n)
            pltpu.make_async_remote_copy(
                src_ref=rolled.at[f, to],
                dst_ref=tall.at[f, me + 2],
                send_sem=send_sem.at[1],
                recv_sem=row_sem.at[f, me],
                device_id={"az": to},
                device_id_type=MESH,
            ).start()

        tall[f, me + 2] = rolled[f, me]

    def await_row(f, j):
        @pl.when(me != j)
        def _():
            got = tall.at[f, j + 2]
            pltpu.make_async_copy(got, got, row_sem.at[f, j]).wait()

    def halo(f, up):
        src, dst, to = (rows, 0, band + 1) if up else (2, rows + 2, band - 1)
        return pltpu.make_async_remote_copy(
            src_ref=tall.at[f, pl.ds(src, 2)],
            dst_ref=tall.at[f, pl.ds(dst, 2)],
            send_sem=halo_send_sem.at[f, int(up)],
            recv_sem=halo_sem.at[f, int(up)],
            device_id={"rad": to},
            device_id_type=MESH,
        )

    def pass_on(f):
        await_row(f, 0)
        await_row(f, 1)
        await_row(f, rows - 2)
        await_row(f, rows - 1)

        @pl.when(jnp.logical_not(first))
        def _():
            halo(f, False).start()

        @pl.when(jnp.logical_not(last))
        def _():
            halo(f, True).start()

    def radial(f):
        for j in range(2, rows - 2):
            await_row(f, j)

        @pl.when(jnp.logical_not(first))
        def _():
            halo(f, True).wait_recv()

        @pl.when(jnp.logical_not(last))
        def _():
            halo(f, False).wait_recv()

        @pl.loop(0, polar // SUB)
        def _(i):
            t = pl.ds(pl.multiple_of(i * SUB, SUB), SUB)
            q = tall[f, :, t, :]
            c = face_rate[:, t, :]
            diff = q[1:] - q[:-1]
            slope = limited(diff[:-1], diff[1:])
            forward = q[1:-2] + 0.5 * (1.0 - c) * slope[:-1]
            backward = q[2:-1] - 0.5 * (1.0 + c) * slope[1:]
            flux = c * jnp.where(c > 0.0, forward, backward)
            result[f, :, t, :] = q[2:-2] - (flux[1:] - flux[:-1])

        pltpu.make_async_copy(result.at[f], out_ref.at[f], store_sem.at[f]).start()

    pass_on(0)

    @pl.loop(1, nf)
    def _(f):
        pass_on(f)
        radial(f - 1)

    radial(nf - 1)

    sent = whole.at[:, pl.ds(0, n - 1)]
    for phase in range(2):
        pltpu.make_async_copy(sent, sent, send_sem.at[phase]).wait()
    for f in range(nf):

        @pl.when(jnp.logical_not(first))
        def _():
            halo(f, False).wait_send()

        @pl.when(jnp.logical_not(last))
        def _():
            halo(f, True).wait_send()

        pltpu.make_async_copy(result.at[f], out_ref.at[f], store_sem.at[f]).wait()


def shards(n, groups, fields, shift, fraction, radial_rate):
    nf, rows, polar, lanes = fields.shape
    assert rows == n and lanes == LANES
    block = lambda *shape: pltpu.VMEM(shape, jnp.float32)
    return pl.pallas_call(
        functools.partial(kernel, n, groups),
        out_shape=jax.ShapeDtypeStruct(fields.shape, jnp.float32),
        in_specs=[
            pl.BlockSpec(memory_space=pltpu.SMEM),
            pl.BlockSpec(memory_space=pltpu.SMEM),
            pl.BlockSpec(memory_space=pl.ANY),
            pl.BlockSpec(memory_space=pl.ANY),
        ],
        out_specs=pl.BlockSpec(memory_space=pl.ANY),
        scratch_shapes=[
            block(nf, rows, polar, LANES),
            block(nf, n, polar, LANES),
            block(n, polar, LANES),
            block(nf, n, polar, LANES),
            block(nf, rows + 4, polar, LANES),
            block(nf, rows, polar, LANES),
            block(min(24, groups * rows), polar),
            block(rows + 1, polar, LANES),
            pltpu.SemaphoreType.DMA((nf,)),
            pltpu.SemaphoreType.DMA,
            pltpu.SemaphoreType.DMA((2,)),
            pltpu.SemaphoreType.DMA((nf,)),
            pltpu.SemaphoreType.DMA((nf, rows)),
            pltpu.SemaphoreType.DMA((nf, 2)),
            pltpu.SemaphoreType.DMA((nf, 2)),
            pltpu.SemaphoreType.DMA((nf,)),
        ],
        compiler_params=pltpu.CompilerParams(collective_id=0, has_side_effects=True),
        name="orbital",
    )(shift, fraction, fields, radial_rate)


def solution(mesh):
    placed = (P(None, "rad", None, "az"), P(), P(), P())
    body = functools.partial(shards, mesh.shape["az"], mesh.shape["rad"])
    return jax.shard_map(
        body, mesh=mesh, in_specs=placed, out_specs=P(None, "rad", None, "az"), check_vma=False
    )
```

```python
import functools

import jax
import jax.numpy as jnp
from jax import lax
from jax.experimental import pallas as pl
from jax.experimental.pallas import tpu as pltpu
from jax.sharding import PartitionSpec as P

MESH = pl.DeviceIdType.MESH
LANES = 128
SUB = 8
AHEAD = 3
VMEM_BYTES = 67043328 - 6000000


def limited(left, right):
    steep = jnp.minimum(
        jnp.minimum(2.0 * jnp.abs(left), 2.0 * jnp.abs(right)), 0.5 * jnp.abs(left + right)
    )
    return jnp.where(left * right > 0.0, jnp.where(left > 0.0, steep, -steep), 0.0)


def blocks_back(x):
    return jnp.concatenate([x[-1:], x[:-1]], axis=0)


def blocks_on(x):
    return jnp.concatenate([x[1:], x[:1]], axis=0)


def kernel(
    n,
    groups,
    shift_ref,
    fraction_ref,
    fields_ref,
    rate_ref,
    out_ref,
    mine,
    whole,
    turned,
    rolled,
    tall,
    shift_smem,
    fraction_smem,
    rate_raw,
    face_rate,
    load_sem,
    rate_sem,
    send_sem,
    gather_sem,
    row_sem,
    halo_send_sem,
    halo_sem,
    go_sem,
    met_sem,
    scalar_sem,
):
    nf, rows, polar, _ = mine.shape
    me = lax.axis_index("az")
    band = lax.axis_index("rad")
    first, last = band == 0, band == groups - 1
    lead, second = n // 2 - 1, n // 2

    edges, others = 4 * nf, rows - 4

    def dealt(slot, device):
        u = slot * n + device
        m, v = lax.rem(u, 4), jnp.maximum(u - edges, 0)
        near = u < edges
        f = jnp.where(near, u // 4, v // others)
        r = jnp.where(near, jnp.where(m >= 2, m + others, m), 2 + lax.rem(v, others))
        return f, r

    def owner(f, r):
        if r < 2:
            u = 4 * f + r
        elif r >= rows - 2:
            u = 4 * f + r - others
        else:
            u = edges + others * f + r - 2
        return lax.rem(u, n)

    for f in range(nf):
        pltpu.make_async_copy(fields_ref.at[f], mine.at[f], load_sem.at[f]).start()
    low = jnp.maximum(band * rows - 1, 0) // LANES * LANES
    low = pl.multiple_of(jnp.minimum(low, rate_ref.shape[1] - rate_raw.shape[1]), LANES)
    rate_copy = pltpu.make_async_copy(
        rate_ref.at[:, pl.ds(low, rate_raw.shape[1])], rate_raw, rate_sem
    )
    rate_copy.start()
    shift_copy = pltpu.make_async_copy(shift_ref, shift_smem, scalar_sem.at[0])
    shift_copy.start()
    fraction_copy = pltpu.make_async_copy(fraction_ref, fraction_smem, scalar_sem.at[1])
    fraction_copy.start()

    barrier = pltpu.get_barrier_semaphore()
    leads = me == lead

    @pl.when(leads)
    def _():
        with jax.named_scope("greet"):
            pl.semaphore_wait(barrier, n - 1)

        @pl.loop(1, n)
        def _(d):
            to = lax.rem(me + d, n)
            pl.semaphore_signal(go_sem, inc=1, device_id={"az": to}, device_id_type=MESH)

    @pl.when(jnp.logical_not(leads))
    def _():
        pl.semaphore_signal(barrier, inc=1, device_id={"az": lead}, device_id_type=MESH)
        with jax.named_scope("greet"):
            pl.semaphore_wait(go_sem, 1)

        @pl.when(jnp.logical_not(first))
        def _():
            pl.semaphore_signal(barrier, inc=1, device_id={"rad": band - 1}, device_id_type=MESH)

        @pl.when(jnp.logical_not(last))
        def _():
            pl.semaphore_signal(barrier, inc=1, device_id={"rad": band + 1}, device_id_type=MESH)

    def meet_neighbours():
        @pl.when(jnp.logical_not(leads))
        def _():
            pl.semaphore_wait(barrier, jnp.where(first, 0, 1) + jnp.where(last, 0, 1))

        @pl.when(me == second)
        def _():
            pl.semaphore_signal(met_sem, inc=1, device_id={"az": lead}, device_id_type=MESH)

        @pl.when(leads)
        def _():
            pl.semaphore_wait(met_sem, 1)

    for f in range(nf):
        pltpu.make_async_copy(fields_ref.at[f], mine.at[f], load_sem.at[f]).wait()

    def gather(s):
        @pl.loop(1, n)
        def _(d):
            to = lax.rem(me + d, n)
            f, r = dealt(s, to)
            pltpu.make_async_remote_copy(
                src_ref=mine.at[f, r],
                dst_ref=whole.at[s, me],
                send_sem=send_sem.at[0],
                recv_sem=gather_sem.at[s],
                device_id={"az": to},
                device_id_type=MESH,
            ).start()

    pl.loop(0, AHEAD)(gather)

    rate_copy.wait()
    at = lax.broadcasted_iota(jnp.int32, rate_raw.shape, 1) + low
    rates = rate_raw[...]
    for i in range(rows + 1):
        here = at == band * rows + i - 1
        column = jnp.sum(jnp.where(here, rates, 0.0), axis=1, keepdims=True)
        if i == 0:
            column = jnp.where(first, 0.0, column)
        if i == rows:
            column = jnp.where(last, 0.0, column)
        face_rate[i] = jnp.broadcast_to(column, (polar, LANES))

    @pl.when(first)
    def _():
        tall[:, 0:2] = jnp.zeros((nf, 2, polar, LANES), jnp.float32)

    @pl.when(last)
    def _():
        tall[:, rows + 2 : rows + 4] = jnp.zeros((nf, 2, polar, LANES), jnp.float32)

    shift_copy.wait()
    fraction_copy.wait()
    lane = lax.broadcasted_iota(jnp.int32, (n, SUB, LANES), 2)
    lane_row = lax.broadcasted_iota(jnp.int32, (polar, LANES), 1)

    def azimuthal(s):
        f, r = dealt(s, me)
        amount = shift_smem[band * rows + r]
        courant = fraction_smem[band * rows + r]
        blocks = amount >> 7
        lanes = amount & (LANES - 1)
        upwind = courant > 0.0
        weight = jnp.where(upwind, 0.5 * (1.0 - courant), -0.5 * (1.0 + courant))
        step = jnp.where(upwind, 1, LANES - 1)
        edge = jnp.where(upwind, 0, LANES - 1)

        whole[s, me] = mine[f, r]
        with jax.named_scope("rows_in"):
            got = whole.at[s, pl.ds(0, n - 1)]
            pltpu.make_async_copy(got, got, gather_sem.at[s]).wait()

        for t in range(0, polar, SUB):
            q = whole[s, :, t : t + SUB, :]
            ahead = pltpu.roll(q, LANES - 1, 2)
            right = jnp.where(lane == LANES - 1, blocks_on(ahead), ahead) - q
            back = pltpu.roll(right, 1, 2)
            left = jnp.where(lane == 0, blocks_back(back), back)
            flux = courant * (q + weight * limited(left, right))
            other = pltpu.roll(flux, step, 2)
            beside = jnp.where(upwind, blocks_back(other), blocks_on(other))
            other = jnp.where(lane == edge, beside, other)
            change = jnp.where(upwind, flux - other, other - flux)
            turned[:, t : t + SUB, :] = pltpu.roll(q - change, lanes, 2)

        @pl.loop(0, n)
        def _(j):
            from_here = lax.rem(j - blocks + n, n)
            from_last = lax.rem(j - blocks - 1 + n + n, n)
            rolled[s, j] = jnp.where(lane_row >= lanes, turned[from_here], turned[from_last])

        tall[f, r + 2] = rolled[s, me]

    def give_back(s):
        f, r = dealt(s, me)

        @pl.loop(1, n)
        def _(d):
            to = lax.rem(me + d, n)
            pltpu.make_async_remote_copy(
                src_ref=rolled.at[s, to],
                dst_ref=tall.at[f, r + 2],
                send_sem=send_sem.at[1],
                recv_sem=row_sem.at[f, r],
                device_id={"az": to},
                device_id_type=MESH,
            ).start()

    def await_row(f, j):
        @pl.when(me != owner(f, j))
        def _():
            got = tall.at[f, j + 2]
            pltpu.make_async_copy(got, got, row_sem.at[f, j]).wait()

    def halo(f, up):
        src, dst, to = (rows, 0, band + 1) if up else (2, rows + 2, band - 1)
        return pltpu.make_async_remote_copy(
            src_ref=tall.at[f, pl.ds(src, 2)],
            dst_ref=tall.at[f, pl.ds(dst, 2)],
            send_sem=halo_send_sem.at[f, int(up)],
            recv_sem=halo_sem.at[f, int(up)],
            device_id={"rad": to},
            device_id_type=MESH,
        )

    def pass_on(f):
        with jax.named_scope("edges_in"):
            await_row(f, 0)
            await_row(f, 1)
            await_row(f, rows - 2)
            await_row(f, rows - 1)

        @pl.when(jnp.logical_not(first))
        def _():
            halo(f, False).start()

        @pl.when(jnp.logical_not(last))
        def _():
            halo(f, True).start()

    def radial(f):
        with jax.named_scope("rest_in"):
            for j in range(2, rows - 2):
                await_row(f, j)

        with jax.named_scope("halo_in"):
            @pl.when(jnp.logical_not(first))
            def _():
                halo(f, True).wait_recv()

            @pl.when(jnp.logical_not(last))
            def _():
                halo(f, False).wait_recv()

        @pl.loop(0, polar // SUB)
        def _(i):
            t = pl.ds(pl.multiple_of(i * SUB, SUB), SUB)
            q = tall[f, :, t, :]
            c = face_rate[:, t, :]
            diff = q[1:] - q[:-1]
            slope = limited(diff[:-1], diff[1:])
            forward = q[1:-2] + 0.5 * (1.0 - c) * slope[:-1]
            backward = q[2:-1] - 0.5 * (1.0 + c) * slope[1:]
            flux = c * jnp.where(c > 0.0, forward, backward)
            out_ref[f, :, t, :] = q[2:-2] - (flux[1:] - flux[:-1])

    early = -(-edges // n)

    @pl.loop(0, early)
    def _(s):
        azimuthal(s)
        give_back(s)

        @pl.when(s + AHEAD < nf)
        def _():
            gather(s + AHEAD)

    pl.loop(early + AHEAD, nf)(gather)
    azimuthal(early)
    with jax.named_scope("meet"):
        meet_neighbours()
    pl.loop(0, nf)(pass_on)
    give_back(early)

    @pl.loop(early + 1, nf)
    def _(s):
        azimuthal(s)
        give_back(s)

    pl.loop(0, nf)(radial)

    with jax.named_scope("finish"):
        sent = whole.at[:, pl.ds(0, n - 1)]
        for phase in range(2):
            pltpu.make_async_copy(sent, sent, send_sem.at[phase]).wait()
        for f in range(nf):

            @pl.when(jnp.logical_not(first))
            def _():
                halo(f, False).wait_send()

            @pl.when(jnp.logical_not(last))
            def _():
                halo(f, True).wait_send()


def shards(n, groups, fields, shift, fraction, radial_rate):
    nf, rows, polar, lanes = fields.shape
    assert rows == n and lanes == LANES
    block = lambda *shape: pltpu.VMEM(shape, jnp.float32)
    return pl.pallas_call(
        functools.partial(kernel, n, groups),
        out_shape=pltpu.VMEM(fields.shape, jnp.float32),
        in_specs=[pl.BlockSpec(memory_space=pltpu.HBM)] * 4,
        out_specs=pl.BlockSpec(memory_space=pltpu.VMEM),
        scratch_shapes=[
            block(nf, rows, polar, LANES),
            block(nf, n, polar, LANES),
            block(n, polar, LANES),
            block(nf, n, polar, LANES),
            block(nf, rows + 4, polar, LANES),
            pltpu.SMEM(shift.shape, jnp.int32),
            pltpu.SMEM(fraction.shape, jnp.float32),
            block(polar, min(2 * LANES, groups * rows)),
            block(rows + 1, polar, LANES),
            pltpu.SemaphoreType.DMA((nf,)),
            pltpu.SemaphoreType.DMA,
            pltpu.SemaphoreType.DMA((2,)),
            pltpu.SemaphoreType.DMA((nf,)),
            pltpu.SemaphoreType.DMA((nf, rows)),
            pltpu.SemaphoreType.DMA((nf, 2)),
            pltpu.SemaphoreType.DMA((nf, 2)),
            pltpu.SemaphoreType.REGULAR,
            pltpu.SemaphoreType.REGULAR,
            pltpu.SemaphoreType.DMA((2,)),
        ],
        compiler_params=pltpu.CompilerParams(
            collective_id=0, has_side_effects=True, vmem_limit_bytes=VMEM_BYTES
        ),
        name="orbital",
    )(shift, fraction, fields, radial_rate.T)


def solution(mesh):
    placed = (P(None, "rad", None, "az"), P(), P(), P())
    body = functools.partial(shards, mesh.shape["az"], mesh.shape["rad"])
    return jax.shard_map(
        body, mesh=mesh, in_specs=placed, out_specs=P(None, "rad", None, "az"), check_vma=False
    )
```

```python
import functools

import jax
import jax.numpy as jnp
from jax import lax
from jax.experimental import pallas as pl
from jax.experimental.pallas import tpu as pltpu
from jax.sharding import PartitionSpec as P

MESH = pl.DeviceIdType.MESH
LANES = 128
SUB = 8
AHEAD = 3
RING = 8
VMEM_BYTES = 67043328 - 6000000


def limited(left, right):
    steep = jnp.minimum(
        jnp.minimum(2.0 * jnp.abs(left), 2.0 * jnp.abs(right)), 0.5 * jnp.abs(left + right)
    )
    return jnp.where(left * right > 0.0, jnp.where(left > 0.0, steep, -steep), 0.0)


def blocks_back(x):
    return jnp.concatenate([x[-1:], x[:-1]], axis=0)


def blocks_on(x):
    return jnp.concatenate([x[1:], x[:1]], axis=0)


def kernel(
    n,
    groups,
    shift_ref,
    fraction_ref,
    fields_ref,
    rate_ref,
    out_ref,
    mine,
    whole,
    turned,
    rolled,
    tall,
    shift_smem,
    fraction_smem,
    rate_raw,
    face_rate,
    load_sem,
    rate_sem,
    send_sem,
    gather_sem,
    row_sem,
    halo_send_sem,
    halo_sem,
    go_sem,
    met_sem,
    scalar_sem,
):
    nf, rows, polar, _ = mine.shape
    me = lax.axis_index("az")
    band = lax.axis_index("rad")
    first, last = band == 0, band == groups - 1
    contact, teller = n - 2, n - 1

    edges, others = 4 * nf, rows - 4
    early = -(-edges // n)

    def dealt(slot, device):
        u = slot * n + device
        m, v = lax.rem(u, 4), jnp.maximum(u - edges, 0)
        near = u < edges
        f = jnp.where(near, u // 4, v // others)
        r = jnp.where(near, jnp.where(m >= 2, m + others, m), 2 + lax.rem(v, others))
        return f, r

    def owner(f, r):
        if r < 2:
            u = 4 * f + r
        elif r >= rows - 2:
            u = 4 * f + r - others
        else:
            u = edges + others * f + r - 2
        return lax.rem(u, n)

    for f in range(nf):
        pltpu.make_async_copy(fields_ref.at[f], mine.at[f], load_sem.at[f]).start()
    low = jnp.maximum(band * rows - 1, 0) // LANES * LANES
    low = pl.multiple_of(jnp.minimum(low, rate_ref.shape[1] - rate_raw.shape[1]), LANES)
    rate_copy = pltpu.make_async_copy(
        rate_ref.at[:, pl.ds(low, rate_raw.shape[1])], rate_raw, rate_sem
    )
    rate_copy.start()
    shift_copy = pltpu.make_async_copy(shift_ref, shift_smem, scalar_sem.at[0])
    shift_copy.start()
    fraction_copy = pltpu.make_async_copy(fraction_ref, fraction_smem, scalar_sem.at[1])
    fraction_copy.start()

    barrier = pltpu.get_barrier_semaphore()
    meets = me == contact

    @pl.loop(1, n)
    def _(d):
        to = lax.rem(me + d, n)

        @pl.when(to != contact)
        def _():
            pl.semaphore_signal(barrier, inc=1, device_id={"az": to}, device_id_type=MESH)

    for f in range(nf):
        pltpu.make_async_copy(fields_ref.at[f], mine.at[f], load_sem.at[f]).wait()

    @pl.loop(0, nf)
    def _(s):
        f, r = dealt(s, me)
        whole[s * n + me] = mine[f, r]

    shift_copy.wait()
    fraction_copy.wait()

    rate_copy.wait()
    at = lax.broadcasted_iota(jnp.int32, rate_raw.shape, 1) + low
    rates = rate_raw[...]
    for i in range(rows + 1):
        here = at == band * rows + i - 1
        rate = jnp.sum(jnp.where(here, rates, 0.0), axis=1, keepdims=True)
        if i == 0:
            rate = jnp.where(first, 0.0, rate)
        if i == rows:
            rate = jnp.where(last, 0.0, rate)
        face_rate[i] = jnp.broadcast_to(rate, (polar, LANES))

    @pl.when(first)
    def _():
        tall[:, 0:2] = jnp.zeros((nf, 2, polar, LANES), jnp.float32)

    @pl.when(last)
    def _():
        tall[:, rows + 2 : rows + 4] = jnp.zeros((nf, 2, polar, LANES), jnp.float32)

    @pl.when(jnp.logical_not(meets))
    def _():
        with jax.named_scope("greet"):
            pl.semaphore_wait(barrier, n - 1)

    @pl.when(me == teller)
    def _():
        pl.semaphore_signal(go_sem, inc=1, device_id={"az": contact}, device_id_type=MESH)

    @pl.when(meets)
    def _():
        with jax.named_scope("greet"):
            pl.semaphore_wait(go_sem, 1)

        @pl.when(jnp.logical_not(first))
        def _():
            pl.semaphore_signal(barrier, inc=1, device_id={"rad": band - 1}, device_id_type=MESH)

        @pl.when(jnp.logical_not(last))
        def _():
            pl.semaphore_signal(barrier, inc=1, device_id={"rad": band + 1}, device_id_type=MESH)

    def meet_neighbours():
        @pl.when(meets)
        def _():
            pl.semaphore_wait(barrier, jnp.where(first, 0, 1) + jnp.where(last, 0, 1))

            @pl.loop(1, n)
            def _(d):
                to = lax.rem(me + d, n)
                pl.semaphore_signal(met_sem, inc=1, device_id={"az": to}, device_id_type=MESH)

        @pl.when(jnp.logical_not(meets))
        def _():
            pl.semaphore_wait(met_sem, 1)

    def gather(s):
        @pl.loop(1, n)
        def _(d):
            to = lax.rem(me + d, n)
            f, r = dealt(s, to)
            pltpu.make_async_remote_copy(
                src_ref=mine.at[f, r],
                dst_ref=whole.at[s * n + me],
                send_sem=send_sem.at[0],
                recv_sem=gather_sem.at[s],
                device_id={"az": to},
                device_id_type=MESH,
            ).start()

    pl.loop(0, AHEAD)(gather)

    lane = lax.broadcasted_iota(jnp.int32, (n, SUB, LANES), 2)
    lane_row = lax.broadcasted_iota(jnp.int32, (polar, LANES), 1)

    def azimuthal(s):
        f, r = dealt(s, me)
        amount = shift_smem[band * rows + r]
        courant = fraction_smem[band * rows + r]
        blocks = amount >> 7
        lanes = amount & (LANES - 1)
        upwind = courant > 0.0
        weight = jnp.where(upwind, 0.5 * (1.0 - courant), -0.5 * (1.0 + courant))
        step = jnp.where(upwind, 1, LANES - 1)
        edge = jnp.where(upwind, 0, LANES - 1)

        with jax.named_scope("rows_in"):
            got = whole.at[pl.ds(s * n, n - 1)]
            pltpu.make_async_copy(got, got, gather_sem.at[s]).wait()

        for t in range(0, polar, SUB):
            q = whole[pl.ds(s * n, n), t : t + SUB, :]
            ahead = pltpu.roll(q, LANES - 1, 2)
            right = jnp.where(lane == LANES - 1, blocks_on(ahead), ahead) - q
            back = pltpu.roll(right, 1, 2)
            left = jnp.where(lane == 0, blocks_back(back), back)
            flux = courant * (q + weight * limited(left, right))
            other = pltpu.roll(flux, step, 2)
            beside = jnp.where(upwind, blocks_back(other), blocks_on(other))
            other = jnp.where(lane == edge, beside, other)
            change = jnp.where(upwind, flux - other, other - flux)
            turned[:, t : t + SUB, :] = pltpu.roll(q - change, lanes, 2)

        @pl.loop(0, n)
        def _(j):
            from_here = lax.rem(j - blocks + n, n)
            from_last = lax.rem(j - blocks - 1 + n + n, n)
            rolled[s * n + j] = jnp.where(lane_row >= lanes, turned[from_here], turned[from_last])

        tall[f, r + 2] = rolled[s * n + me]

    def give_back(s):
        f, r = dealt(s, me)

        @pl.loop(1, n)
        def _(d):
            to = lax.rem(me + d, n)
            pltpu.make_async_remote_copy(
                src_ref=rolled.at[s * n + to],
                dst_ref=tall.at[f, r + 2],
                send_sem=send_sem.at[1],
                recv_sem=row_sem.at[f, r],
                device_id={"az": to},
                device_id_type=MESH,
            ).start()

    def await_row(f, j):
        @pl.when(me != owner(f, j))
        def _():
            got = tall.at[f, j + 2]
            pltpu.make_async_copy(got, got, row_sem.at[f, j]).wait()

    def halo(f, up):
        src, dst, to = (rows, 0, band + 1) if up else (2, rows + 2, band - 1)
        return pltpu.make_async_remote_copy(
            src_ref=tall.at[f, pl.ds(src, 2)],
            dst_ref=tall.at[f, pl.ds(dst, 2)],
            send_sem=halo_send_sem.at[f, int(up)],
            recv_sem=halo_sem.at[f, int(up)],
            device_id={"rad": to},
            device_id_type=MESH,
        )

    def pass_on(f):
        with jax.named_scope("edges_in"):
            await_row(f, 0)
            await_row(f, 1)
            await_row(f, rows - 2)
            await_row(f, rows - 1)

        @pl.when(jnp.logical_not(first))
        def _():
            halo(f, False).start()

        @pl.when(jnp.logical_not(last))
        def _():
            halo(f, True).start()

    def radial(f):
        with jax.named_scope("rest_in"):
            for j in range(2, rows - 2):
                await_row(f, j)

        with jax.named_scope("halo_in"):
            @pl.when(jnp.logical_not(first))
            def _():
                halo(f, True).wait_recv()

            @pl.when(jnp.logical_not(last))
            def _():
                halo(f, False).wait_recv()

        @pl.loop(0, polar // SUB)
        def _(i):
            t = pl.ds(pl.multiple_of(i * SUB, SUB), SUB)
            q = tall[f, :, t, :]
            c = face_rate[:, t, :]
            diff = q[1:] - q[:-1]
            slope = limited(diff[:-1], diff[1:])
            forward = q[1:-2] + 0.5 * (1.0 - c) * slope[:-1]
            backward = q[2:-1] - 0.5 * (1.0 + c) * slope[1:]
            flux = c * jnp.where(c > 0.0, forward, backward)
            out_ref[f, :, t, :] = q[2:-2] - (flux[1:] - flux[:-1])

    hold = lax.rem(band, RING) >= RING - 2

    def halos():
        with jax.named_scope("meet"):
            meet_neighbours()
        pl.loop(0, nf)(pass_on)

    @pl.loop(0, nf)
    def _(s):
        azimuthal(s)

        @pl.when(hold & (s == early))
        def _():
            halos()

        give_back(s)

        @pl.when(jnp.logical_not(hold) & (s == early))
        def _():
            halos()

        @pl.loop(s + AHEAD, jnp.where(s == early - 1, nf, jnp.minimum(s + AHEAD + 1, nf)))
        def _(later):
            @pl.when(s < early)
            def _():
                gather(later)

    pl.loop(0, nf)(radial)

    with jax.named_scope("finish"):
        for phase in range(2):
            sent = whole.at[pl.ds(0, nf * (n - 1))]
            pltpu.make_async_copy(sent, sent, send_sem.at[phase]).wait()

        for f in range(nf):

            @pl.when(jnp.logical_not(first))
            def _():
                halo(f, False).wait_send()

            @pl.when(jnp.logical_not(last))
            def _():
                halo(f, True).wait_send()


def shards(n, groups, fields, shift, fraction, radial_rate):
    nf, rows, polar, lanes = fields.shape
    assert rows == n and lanes == LANES and rows >= 4
    block = lambda *shape: pltpu.VMEM(shape, jnp.float32)
    return pl.pallas_call(
        functools.partial(kernel, n, groups),
        out_shape=pltpu.VMEM(fields.shape, jnp.float32),
        in_specs=[pl.BlockSpec(memory_space=pltpu.HBM)] * 4,
        out_specs=pl.BlockSpec(memory_space=pltpu.VMEM),
        scratch_shapes=[
            block(nf, rows, polar, LANES),
            block(nf * n, polar, LANES),
            block(n, polar, LANES),
            block(nf * n, polar, LANES),
            block(nf, rows + 4, polar, LANES),
            pltpu.SMEM(shift.shape, jnp.int32),
            pltpu.SMEM(fraction.shape, jnp.float32),
            block(polar, min(2 * LANES, groups * rows)),
            block(rows + 1, polar, LANES),
            pltpu.SemaphoreType.DMA((nf,)),
            pltpu.SemaphoreType.DMA,
            pltpu.SemaphoreType.DMA((2,)),
            pltpu.SemaphoreType.DMA((nf,)),
            pltpu.SemaphoreType.DMA((nf, rows)),
            pltpu.SemaphoreType.DMA((nf, 2)),
            pltpu.SemaphoreType.DMA((nf, 2)),
            pltpu.SemaphoreType.REGULAR,
            pltpu.SemaphoreType.REGULAR,
            pltpu.SemaphoreType.DMA((2,)),
        ],
        compiler_params=pltpu.CompilerParams(
            collective_id=0, has_side_effects=True, vmem_limit_bytes=VMEM_BYTES
        ),
        name="orbital",
    )(shift, fraction, fields, radial_rate.T)


def solution(mesh):
    placed = (P(None, "rad", None, "az"), P(), P(), P())
    body = functools.partial(shards, mesh.shape["az"], mesh.shape["rad"])
    return jax.shard_map(
        body, mesh=mesh, in_specs=placed, out_specs=P(None, "rad", None, "az"), check_vma=False
    )
```

```python
import functools

import jax
import jax.numpy as jnp
from jax import lax
from jax.experimental import pallas as pl
from jax.experimental.pallas import tpu as pltpu
from jax.sharding import PartitionSpec as P

MESH = pl.DeviceIdType.MESH
LANES = 128
SUB = 8
AHEAD = 3
VMEM_BYTES = 67043328 - 6000000


def limited(left, right):
    steep = jnp.minimum(
        jnp.minimum(2.0 * jnp.abs(left), 2.0 * jnp.abs(right)), 0.5 * jnp.abs(left + right)
    )
    return jnp.where(left * right > 0.0, jnp.where(left > 0.0, steep, -steep), 0.0)


def blocks_back(x):
    return jnp.concatenate([x[-1:], x[:-1]], axis=0)


def blocks_on(x):
    return jnp.concatenate([x[1:], x[:1]], axis=0)


def kernel(
    n,
    groups,
    shift_ref,
    fraction_ref,
    fields_ref,
    rate_ref,
    out_ref,
    mine,
    whole,
    turned,
    rolled,
    tall,
    shift_smem,
    fraction_smem,
    rate_raw,
    face_rate,
    load_sem,
    rate_sem,
    send_sem,
    gather_sem,
    row_sem,
    halo_send_sem,
    halo_sem,
    go_sem,
    met_sem,
    scalar_sem,
):
    nf, rows, polar, _ = mine.shape
    me = lax.axis_index("az")
    band = lax.axis_index("rad")
    first, last = band == 0, band == groups - 1
    contact, teller = n - 2, n - 1

    third = n // 3
    near, others = 2 * nf, rows - 4
    early = 2
    upper = lax.rem(band, 2) == 1
    seat = jnp.where(upper, n - 1 - me, me)
    far_base = jnp.where(upper, rows - 2, 0)
    near_base = jnp.where(upper, 0, rows - 2)
    far_there = jnp.where(upper, jnp.logical_not(last), jnp.logical_not(first))
    far_band = jnp.where(upper, band + 1, band - 1)
    far_row = jnp.where(upper, 0, rows + 2)
    spare = 2 * nf - 2 * third
    far_count = jnp.where(seat < third, 2, jnp.where(seat < third + spare, 1, 0))

    def dealt(slot, device):
        at = jnp.where(upper, n - 1 - device, device)
        in_first = slot == 0
        is_far = at < jnp.where(in_first, third, third + spare)
        c = jnp.where(is_far, at + slot * third, at - jnp.where(in_first, third, spare - third))
        u = slot * n + at
        v = jnp.maximum(u - 4 * nf, 0)
        edge = u < 4 * nf
        f = jnp.where(edge, c // 2, v // others)
        base = jnp.where(is_far, far_base, near_base)
        r = jnp.where(edge, base + lax.rem(c, 2), 2 + lax.rem(v, others))
        return f, r

    def owner(f, r):
        c = 2 * f + (r if r < 2 else r - others - 2)
        is_far = upper if r >= rows - 2 else jnp.logical_not(upper)
        if 2 <= r < rows - 2:
            at = lax.rem(4 * nf + others * f + r - 2, n)
        else:
            far_at = jnp.where(c < third, c, c - third)
            near_at = jnp.where(c < 2 * third, c + third, c + spare - third)
            at = jnp.where(is_far, far_at, near_at)
        return jnp.where(upper, n - 1 - at, at)

    for f in range(nf):
        pltpu.make_async_copy(fields_ref.at[f], mine.at[f], load_sem.at[f]).start()
    low = jnp.maximum(band * rows - 1, 0) // LANES * LANES
    low = pl.multiple_of(jnp.minimum(low, rate_ref.shape[1] - rate_raw.shape[1]), LANES)
    rate_copy = pltpu.make_async_copy(
        rate_ref.at[:, pl.ds(low, rate_raw.shape[1])], rate_raw, rate_sem
    )
    rate_copy.start()
    shift_copy = pltpu.make_async_copy(shift_ref, shift_smem, scalar_sem.at[0])
    shift_copy.start()
    fraction_copy = pltpu.make_async_copy(fraction_ref, fraction_smem, scalar_sem.at[1])
    fraction_copy.start()

    barrier = pltpu.get_barrier_semaphore()
    meets = me == contact

    @pl.loop(1, n)
    def _(d):
        to = lax.rem(me + d, n)

        @pl.when(to != contact)
        def _():
            pl.semaphore_signal(barrier, inc=1, device_id={"az": to}, device_id_type=MESH)

    for f in range(nf):
        pltpu.make_async_copy(fields_ref.at[f], mine.at[f], load_sem.at[f]).wait()

    @pl.loop(0, nf)
    def _(s):
        f, r = dealt(s, me)
        whole[s * n + me] = mine[f, r]

    shift_copy.wait()
    fraction_copy.wait()

    rate_copy.wait()
    at = lax.broadcasted_iota(jnp.int32, rate_raw.shape, 1) + low
    rates = rate_raw[...]
    for i in range(rows + 1):
        here = at == band * rows + i - 1
        rate = jnp.sum(jnp.where(here, rates, 0.0), axis=1, keepdims=True)
        if i == 0:
            rate = jnp.where(first, 0.0, rate)
        if i == rows:
            rate = jnp.where(last, 0.0, rate)
        face_rate[i] = jnp.broadcast_to(rate, (polar, LANES))

    @pl.when(first)
    def _():
        tall[:, 0:2] = jnp.zeros((nf, 2, polar, LANES), jnp.float32)

    @pl.when(last)
    def _():
        tall[:, rows + 2 : rows + 4] = jnp.zeros((nf, 2, polar, LANES), jnp.float32)

    @pl.when(jnp.logical_not(meets))
    def _():
        with jax.named_scope("greet"):
            pl.semaphore_wait(barrier, n - 1)

    @pl.when(me == teller)
    def _():
        pl.semaphore_signal(go_sem, inc=1, device_id={"az": contact}, device_id_type=MESH)

    @pl.when(meets)
    def _():
        with jax.named_scope("greet"):
            pl.semaphore_wait(go_sem, 1)

        @pl.when(jnp.logical_not(first))
        def _():
            pl.semaphore_signal(barrier, inc=1, device_id={"rad": band - 1}, device_id_type=MESH)

        @pl.when(jnp.logical_not(last))
        def _():
            pl.semaphore_signal(barrier, inc=1, device_id={"rad": band + 1}, device_id_type=MESH)

    def meet_neighbours():
        @pl.when(meets)
        def _():
            pl.semaphore_wait(barrier, jnp.where(first, 0, 1) + jnp.where(last, 0, 1))

            @pl.loop(1, n)
            def _(d):
                to = lax.rem(me + d, n)
                pl.semaphore_signal(met_sem, inc=1, device_id={"az": to}, device_id_type=MESH)

        @pl.when(jnp.logical_not(meets))
        def _():
            pl.semaphore_wait(met_sem, 1)

    def gather(s):
        @pl.loop(1, n)
        def _(d):
            to = lax.rem(me + d, n)
            f, r = dealt(s, to)
            pltpu.make_async_remote_copy(
                src_ref=mine.at[f, r],
                dst_ref=whole.at[s * n + me],
                send_sem=send_sem.at[0],
                recv_sem=gather_sem.at[s],
                device_id={"az": to},
                device_id_type=MESH,
            ).start()

    pl.loop(0, AHEAD)(gather)

    lane = lax.broadcasted_iota(jnp.int32, (n, SUB, LANES), 2)
    lane_row = lax.broadcasted_iota(jnp.int32, (polar, LANES), 1)

    def azimuthal(s):
        f, r = dealt(s, me)
        amount = shift_smem[band * rows + r]
        courant = fraction_smem[band * rows + r]
        blocks = amount >> 7
        lanes = amount & (LANES - 1)
        upwind = courant > 0.0
        weight = jnp.where(upwind, 0.5 * (1.0 - courant), -0.5 * (1.0 + courant))
        step = jnp.where(upwind, 1, LANES - 1)
        edge = jnp.where(upwind, 0, LANES - 1)

        with jax.named_scope("rows_in"):
            got = whole.at[pl.ds(s * n, n - 1)]
            pltpu.make_async_copy(got, got, gather_sem.at[s]).wait()

        for t in range(0, polar, SUB):
            q = whole[pl.ds(s * n, n), t : t + SUB, :]
            ahead = pltpu.roll(q, LANES - 1, 2)
            right = jnp.where(lane == LANES - 1, blocks_on(ahead), ahead) - q
            back = pltpu.roll(right, 1, 2)
            left = jnp.where(lane == 0, blocks_back(back), back)
            flux = courant * (q + weight * limited(left, right))
            other = pltpu.roll(flux, step, 2)
            beside = jnp.where(upwind, blocks_back(other), blocks_on(other))
            other = jnp.where(lane == edge, beside, other)
            change = jnp.where(upwind, flux - other, other - flux)
            turned[:, t : t + SUB, :] = pltpu.roll(q - change, lanes, 2)

        @pl.loop(0, n)
        def _(j):
            from_here = lax.rem(j - blocks + n, n)
            from_last = lax.rem(j - blocks - 1 + n + n, n)
            rolled[s * n + j] = jnp.where(lane_row >= lanes, turned[from_here], turned[from_last])

        tall[f, r + 2] = rolled[s * n + me]

    def give_back(s):
        f, r = dealt(s, me)

        @pl.loop(1, n)
        def _(d):
            to = lax.rem(me + d, n)
            pltpu.make_async_remote_copy(
                src_ref=rolled.at[s * n + to],
                dst_ref=tall.at[f, r + 2],
                send_sem=send_sem.at[1],
                recv_sem=row_sem.at[f, r],
                device_id={"az": to},
                device_id_type=MESH,
            ).start()

    def await_row(f, j):
        @pl.when(me != owner(f, j))
        def _():
            got = tall.at[f, j + 2]
            pltpu.make_async_copy(got, got, row_sem.at[f, j]).wait()

    def send_far():
        @pl.loop(2 - far_count, 2)
        def _(s):
            f, r = dealt(s, me)

            @pl.loop(0, n)
            def _(d):
                to = lax.rem(me + d, n)
                pltpu.make_async_remote_copy(
                    src_ref=rolled.at[s * n + to],
                    dst_ref=tall.at[f, far_row + r - far_base],
                    send_sem=halo_send_sem.at[0],
                    recv_sem=halo_sem.at[f, 0],
                    device_id={"az": to, "rad": far_band},
                    device_id_type=MESH,
                ).start()

    def near_halo(f, up):
        src, dst, to = (rows, 0, band + 1) if up else (2, rows + 2, band - 1)
        return pltpu.make_async_remote_copy(
            src_ref=tall.at[f, pl.ds(src, 2)],
            dst_ref=tall.at[f, pl.ds(dst, 2)],
            send_sem=halo_send_sem.at[1],
            recv_sem=halo_sem.at[f, 1],
            device_id={"rad": to},
            device_id_type=MESH,
        )

    def pass_on(f):
        @pl.when(upper)
        def _():
            await_row(f, 0)
            await_row(f, 1)
            near_halo(f, False).start()

        @pl.when(jnp.logical_not(upper))
        def _():
            await_row(f, rows - 2)
            await_row(f, rows - 1)
            near_halo(f, True).start()

    def radial(f):
        with jax.named_scope("rest_in"):
            @pl.when(upper)
            def _():
                await_row(f, rows - 2)
                await_row(f, rows - 1)

            @pl.when(jnp.logical_not(upper))
            def _():
                await_row(f, 0)
                await_row(f, 1)

            for j in range(2, rows - 2):
                await_row(f, j)

        with jax.named_scope("halo_in"):
            two = tall.at[f, pl.ds(0, 2)]

            @pl.when(far_there)
            def _():
                pltpu.make_async_copy(two, two, halo_sem.at[f, 0]).wait()

            pltpu.make_async_copy(two, two, halo_sem.at[f, 1]).wait()

        @pl.loop(0, polar // SUB)
        def _(i):
            t = pl.ds(pl.multiple_of(i * SUB, SUB), SUB)
            q = tall[f, :, t, :]
            c = face_rate[:, t, :]
            diff = q[1:] - q[:-1]
            slope = limited(diff[:-1], diff[1:])
            forward = q[1:-2] + 0.5 * (1.0 - c) * slope[:-1]
            backward = q[2:-1] - 0.5 * (1.0 + c) * slope[1:]
            flux = c * jnp.where(c > 0.0, forward, backward)
            out_ref[f, :, t, :] = q[2:-2] - (flux[1:] - flux[:-1])

    @pl.loop(0, nf)
    def _(s):
        azimuthal(s)

        @pl.when(s == early)
        def _():
            with jax.named_scope("meet"):
                meet_neighbours()
            pl.when(far_there)(send_far)

        give_back(s)

        @pl.when(s == early)
        def _():
            pl.loop(0, nf)(pass_on)

        @pl.loop(s + AHEAD, jnp.where(s == early - 1, nf, jnp.minimum(s + AHEAD + 1, nf)))
        def _(later):
            @pl.when(s < early)
            def _():
                gather(later)

    pl.loop(0, nf)(radial)

    with jax.named_scope("finish"):
        for phase in range(2):
            sent = whole.at[pl.ds(0, nf * (n - 1))]
            pltpu.make_async_copy(sent, sent, send_sem.at[phase]).wait()

        for units in (1, 2):

            @pl.when(far_there & (far_count == units))
            def _():
                sent = rolled.at[pl.ds(0, units * n)]
                pltpu.make_async_copy(sent, sent, halo_send_sem.at[0]).wait()

        sent = rolled.at[pl.ds(0, 2 * nf)]
        pltpu.make_async_copy(sent, sent, halo_send_sem.at[1]).wait()


def shards(n, groups, fields, shift, fraction, radial_rate):
    nf, rows, polar, lanes = fields.shape
    assert rows == n == 12 and lanes == LANES and nf == 5 and groups % 2 == 0
    block = lambda *shape: pltpu.VMEM(shape, jnp.float32)
    return pl.pallas_call(
        functools.partial(kernel, n, groups),
        out_shape=pltpu.VMEM(fields.shape, jnp.float32),
        in_specs=[pl.BlockSpec(memory_space=pltpu.HBM)] * 4,
        out_specs=pl.BlockSpec(memory_space=pltpu.VMEM),
        scratch_shapes=[
            block(nf, rows, polar, LANES),
            block(nf * n, polar, LANES),
            block(n, polar, LANES),
            block(nf * n, polar, LANES),
            block(nf, rows + 4, polar, LANES),
            pltpu.SMEM(shift.shape, jnp.int32),
            pltpu.SMEM(fraction.shape, jnp.float32),
            block(polar, min(2 * LANES, groups * rows)),
            block(rows + 1, polar, LANES),
            pltpu.SemaphoreType.DMA((nf,)),
            pltpu.SemaphoreType.DMA,
            pltpu.SemaphoreType.DMA((2,)),
            pltpu.SemaphoreType.DMA((nf,)),
            pltpu.SemaphoreType.DMA((nf, rows)),
            pltpu.SemaphoreType.DMA((2,)),
            pltpu.SemaphoreType.DMA((nf, 2)),
            pltpu.SemaphoreType.REGULAR,
            pltpu.SemaphoreType.REGULAR,
            pltpu.SemaphoreType.DMA((2,)),
        ],
        compiler_params=pltpu.CompilerParams(
            collective_id=0, has_side_effects=True, vmem_limit_bytes=VMEM_BYTES
        ),
        name="orbital",
    )(shift, fraction, fields, radial_rate.T)


def solution(mesh):
    placed = (P(None, "rad", None, "az"), P(), P(), P())
    body = functools.partial(shards, mesh.shape["az"], mesh.shape["rad"])
    return jax.shard_map(
        body, mesh=mesh, in_specs=placed, out_specs=P(None, "rad", None, "az"), check_vma=False
    )
```

```python
import functools

import jax
import jax.numpy as jnp
from jax import lax
from jax.experimental import pallas as pl
from jax.experimental.pallas import tpu as pltpu
from jax.sharding import PartitionSpec as P

MESH = pl.DeviceIdType.MESH
LANES = 128
SUB = 8
AHEAD = 3
VMEM_BYTES = 67043328 - 6000000


def limited(left, right):
    steep = jnp.minimum(
        jnp.minimum(2.0 * jnp.abs(left), 2.0 * jnp.abs(right)), 0.5 * jnp.abs(left + right)
    )
    return jnp.where(left * right > 0.0, jnp.where(left > 0.0, steep, -steep), 0.0)


def blocks_back(x):
    return jnp.concatenate([x[-1:], x[:-1]], axis=0)


def blocks_on(x):
    return jnp.concatenate([x[1:], x[:1]], axis=0)


def kernel(
    n,
    groups,
    shift_ref,
    fraction_ref,
    fields_ref,
    rate_ref,
    out_ref,
    mine,
    whole,
    turned,
    rolled,
    tall,
    shift_smem,
    fraction_smem,
    rate_raw,
    face_rate,
    load_sem,
    rate_sem,
    send_sem,
    gather_sem,
    row_sem,
    halo_send_sem,
    halo_sem,
    go_sem,
    met_sem,
    scalar_sem,
):
    nf, rows, polar, _ = mine.shape
    me = lax.axis_index("az")
    band = lax.axis_index("rad")
    first, last = band == 0, band == groups - 1
    contact, teller = n - 2, n - 1

    third = n // 3
    near, others = 2 * nf, rows - 4
    early = 2
    upper = lax.rem(band, 2) == 1
    seat = jnp.where(upper, n - 1 - me, me)
    far_base = jnp.where(upper, rows - 2, 0)
    near_base = jnp.where(upper, 0, rows - 2)
    far_there = jnp.where(upper, jnp.logical_not(last), jnp.logical_not(first))
    far_band = jnp.where(upper, band + 1, band - 1)
    far_row = jnp.where(upper, 0, rows + 2)
    spare = 2 * nf - 2 * third
    far_count = jnp.where(seat < third, 2, jnp.where(seat < third + spare, 1, 0))

    def dealt(slot, device):
        at = jnp.where(upper, n - 1 - device, device)
        in_first = slot == 0
        is_far = at < jnp.where(in_first, third, third + spare)
        c = jnp.where(is_far, at + slot * third, at - jnp.where(in_first, third, spare - third))
        u = slot * n + at
        v = jnp.maximum(u - 4 * nf, 0)
        edge = u < 4 * nf
        f = jnp.where(edge, c // 2, v // others)
        base = jnp.where(is_far, far_base, near_base)
        r = jnp.where(edge, base + lax.rem(c, 2), 2 + lax.rem(v, others))
        return f, r

    def owner(f, r):
        c = 2 * f + (r if r < 2 else r - others - 2)
        is_far = upper if r >= rows - 2 else jnp.logical_not(upper)
        if 2 <= r < rows - 2:
            at = lax.rem(4 * nf + others * f + r - 2, n)
        else:
            far_at = jnp.where(c < third, c, c - third)
            near_at = jnp.where(c < 2 * third, c + third, c + spare - third)
            at = jnp.where(is_far, far_at, near_at)
        return jnp.where(upper, n - 1 - at, at)

    for f in range(nf):
        pltpu.make_async_copy(fields_ref.at[f], mine.at[f], load_sem.at[f]).start()
    low = jnp.maximum(band * rows - 1, 0) // LANES * LANES
    low = pl.multiple_of(jnp.minimum(low, rate_ref.shape[1] - rate_raw.shape[1]), LANES)
    rate_copy = pltpu.make_async_copy(
        rate_ref.at[:, pl.ds(low, rate_raw.shape[1])], rate_raw, rate_sem
    )
    rate_copy.start()
    shift_copy = pltpu.make_async_copy(shift_ref, shift_smem, scalar_sem.at[0])
    shift_copy.start()
    fraction_copy = pltpu.make_async_copy(fraction_ref, fraction_smem, scalar_sem.at[1])
    fraction_copy.start()

    barrier = pltpu.get_barrier_semaphore()
    meets = me == contact

    @pl.loop(1, n)
    def _(d):
        to = lax.rem(me + d, n)

        @pl.when(to != contact)
        def _():
            pl.semaphore_signal(barrier, inc=1, device_id={"az": to}, device_id_type=MESH)

    for f in range(nf):
        pltpu.make_async_copy(fields_ref.at[f], mine.at[f], load_sem.at[f]).wait()

    @pl.loop(0, nf)
    def _(s):
        f, r = dealt(s, me)
        whole[s * n + me] = mine[f, r]

    shift_copy.wait()
    fraction_copy.wait()

    rate_copy.wait()
    at = lax.broadcasted_iota(jnp.int32, rate_raw.shape, 1) + low
    rates = rate_raw[...]
    for i in range(rows + 1):
        here = at == band * rows + i - 1
        rate = jnp.sum(jnp.where(here, rates, 0.0), axis=1, keepdims=True)
        if i == 0:
            rate = jnp.where(first, 0.0, rate)
        if i == rows:
            rate = jnp.where(last, 0.0, rate)
        face_rate[i] = jnp.broadcast_to(rate, (polar, LANES))

    @pl.when(first)
    def _():
        tall[:, 0:2] = jnp.zeros((nf, 2, polar, LANES), jnp.float32)

    @pl.when(last)
    def _():
        tall[:, rows + 2 : rows + 4] = jnp.zeros((nf, 2, polar, LANES), jnp.float32)

    @pl.when(jnp.logical_not(meets))
    def _():
        with jax.named_scope("greet"):
            pl.semaphore_wait(barrier, n - 1)

    @pl.when(me == teller)
    def _():
        pl.semaphore_signal(go_sem, inc=1, device_id={"az": contact}, device_id_type=MESH)

    @pl.when(meets)
    def _():
        with jax.named_scope("greet"):
            pl.semaphore_wait(go_sem, 1)

        @pl.when(jnp.logical_not(first))
        def _():
            pl.semaphore_signal(barrier, inc=1, device_id={"rad": band - 1}, device_id_type=MESH)

        @pl.when(jnp.logical_not(last))
        def _():
            pl.semaphore_signal(barrier, inc=1, device_id={"rad": band + 1}, device_id_type=MESH)

    def meet_neighbours():
        @pl.when(meets)
        def _():
            pl.semaphore_wait(barrier, jnp.where(first, 0, 1) + jnp.where(last, 0, 1))

            @pl.loop(1, n)
            def _(d):
                to = lax.rem(me + d, n)
                pl.semaphore_signal(met_sem, inc=1, device_id={"az": to}, device_id_type=MESH)

    def await_meeting():
        @pl.when(jnp.logical_not(meets))
        def _():
            pl.semaphore_wait(met_sem, 1)

    def gather(s):
        @pl.loop(1, n)
        def _(d):
            to = lax.rem(me + d, n)
            f, r = dealt(s, to)
            pltpu.make_async_remote_copy(
                src_ref=mine.at[f, r],
                dst_ref=whole.at[s * n + me],
                send_sem=send_sem.at[0],
                recv_sem=gather_sem.at[s],
                device_id={"az": to},
                device_id_type=MESH,
            ).start()

    pl.loop(0, AHEAD)(gather)

    lane = lax.broadcasted_iota(jnp.int32, (n, SUB, LANES), 2)
    lane_row = lax.broadcasted_iota(jnp.int32, (polar, LANES), 1)

    def azimuthal(s):
        f, r = dealt(s, me)
        amount = shift_smem[band * rows + r]
        courant = fraction_smem[band * rows + r]
        blocks = amount >> 7
        lanes = amount & (LANES - 1)
        upwind = courant > 0.0
        weight = jnp.where(upwind, 0.5 * (1.0 - courant), -0.5 * (1.0 + courant))
        step = jnp.where(upwind, 1, LANES - 1)
        edge = jnp.where(upwind, 0, LANES - 1)

        with jax.named_scope("rows_in"):
            got = whole.at[pl.ds(s * n, n - 1)]
            pltpu.make_async_copy(got, got, gather_sem.at[s]).wait()

        for t in range(0, polar, SUB):
            q = whole[pl.ds(s * n, n), t : t + SUB, :]
            ahead = pltpu.roll(q, LANES - 1, 2)
            right = jnp.where(lane == LANES - 1, blocks_on(ahead), ahead) - q
            back = pltpu.roll(right, 1, 2)
            left = jnp.where(lane == 0, blocks_back(back), back)
            flux = courant * (q + weight * limited(left, right))
            other = pltpu.roll(flux, step, 2)
            beside = jnp.where(upwind, blocks_back(other), blocks_on(other))
            other = jnp.where(lane == edge, beside, other)
            change = jnp.where(upwind, flux - other, other - flux)
            turned[:, t : t + SUB, :] = pltpu.roll(q - change, lanes, 2)

        @pl.loop(0, n)
        def _(j):
            from_here = lax.rem(j - blocks + n, n)
            from_last = lax.rem(j - blocks - 1 + n + n, n)
            rolled[s * n + j] = jnp.where(lane_row >= lanes, turned[from_here], turned[from_last])

        tall[f, r + 2] = rolled[s * n + me]

    def give_back(s):
        f, r = dealt(s, me)

        @pl.loop(1, n)
        def _(d):
            to = lax.rem(me + d, n)
            pltpu.make_async_remote_copy(
                src_ref=rolled.at[s * n + to],
                dst_ref=tall.at[f, r + 2],
                send_sem=send_sem.at[1],
                recv_sem=row_sem.at[f, r],
                device_id={"az": to},
                device_id_type=MESH,
            ).start()

    def await_row(f, j):
        @pl.when(me != owner(f, j))
        def _():
            got = tall.at[f, j + 2]
            pltpu.make_async_copy(got, got, row_sem.at[f, j]).wait()

    def send_far():
        @pl.loop(2 - far_count, 2)
        def _(s):
            f, r = dealt(s, me)

            @pl.loop(0, n)
            def _(d):
                to = lax.rem(me + d, n)
                pltpu.make_async_remote_copy(
                    src_ref=rolled.at[s * n + to],
                    dst_ref=tall.at[f, far_row + r - far_base],
                    send_sem=halo_send_sem.at[0],
                    recv_sem=halo_sem.at[f, 0],
                    device_id={"az": to, "rad": far_band},
                    device_id_type=MESH,
                ).start()

    def near_halo(f, up):
        src, dst, to = (rows, 0, band + 1) if up else (2, rows + 2, band - 1)
        return pltpu.make_async_remote_copy(
            src_ref=tall.at[f, pl.ds(src, 2)],
            dst_ref=tall.at[f, pl.ds(dst, 2)],
            send_sem=halo_send_sem.at[1],
            recv_sem=halo_sem.at[f, 1],
            device_id={"rad": to},
            device_id_type=MESH,
        )

    def pass_on(f):
        @pl.when(upper)
        def _():
            await_row(f, 0)
            await_row(f, 1)
            near_halo(f, False).start()

        @pl.when(jnp.logical_not(upper))
        def _():
            await_row(f, rows - 2)
            await_row(f, rows - 1)
            near_halo(f, True).start()

    def radial(f):
        with jax.named_scope("rest_in"):
            @pl.when(upper)
            def _():
                await_row(f, rows - 2)
                await_row(f, rows - 1)

            @pl.when(jnp.logical_not(upper))
            def _():
                await_row(f, 0)
                await_row(f, 1)

            for j in range(2, rows - 2):
                await_row(f, j)

        with jax.named_scope("halo_in"):
            two = tall.at[f, pl.ds(0, 2)]

            @pl.when(far_there)
            def _():
                pltpu.make_async_copy(two, two, halo_sem.at[f, 0]).wait()

            pltpu.make_async_copy(two, two, halo_sem.at[f, 1]).wait()

        @pl.loop(0, polar // SUB)
        def _(i):
            t = pl.ds(pl.multiple_of(i * SUB, SUB), SUB)
            q = tall[f, :, t, :]
            c = face_rate[:, t, :]
            diff = q[1:] - q[:-1]
            slope = limited(diff[:-1], diff[1:])
            forward = q[1:-2] + 0.5 * (1.0 - c) * slope[:-1]
            backward = q[2:-1] - 0.5 * (1.0 + c) * slope[1:]
            flux = c * jnp.where(c > 0.0, forward, backward)
            out_ref[f, :, t, :] = q[2:-2] - (flux[1:] - flux[:-1])

    @pl.loop(0, nf)
    def _(s):
        azimuthal(s)

        @pl.when(s == early)
        def _():
            with jax.named_scope("meet"):
                await_meeting()
            pl.when(far_there)(send_far)

        give_back(s)
        pl.when(s == early - 1)(meet_neighbours)

        @pl.when(s == early)
        def _():
            pl.loop(0, nf)(pass_on)

        @pl.loop(s + AHEAD, jnp.where(s == early - 1, nf, jnp.minimum(s + AHEAD + 1, nf)))
        def _(later):
            @pl.when(s < early)
            def _():
                gather(later)

    pl.loop(0, nf)(radial)

    with jax.named_scope("finish"):
        for phase in range(2):
            sent = whole.at[pl.ds(0, nf * (n - 1))]
            pltpu.make_async_copy(sent, sent, send_sem.at[phase]).wait()

        for units in (1, 2):

            @pl.when(far_there & (far_count == units))
            def _():
                sent = rolled.at[pl.ds(0, units * n)]
                pltpu.make_async_copy(sent, sent, halo_send_sem.at[0]).wait()

        sent = rolled.at[pl.ds(0, 2 * nf)]
        pltpu.make_async_copy(sent, sent, halo_send_sem.at[1]).wait()


def shards(n, groups, fields, shift, fraction, radial_rate):
    nf, rows, polar, lanes = fields.shape
    assert rows == n == 12 and lanes == LANES and nf == 5 and groups % 2 == 0
    block = lambda *shape: pltpu.VMEM(shape, jnp.float32)
    return pl.pallas_call(
        functools.partial(kernel, n, groups),
        out_shape=pltpu.VMEM(fields.shape, jnp.float32),
        in_specs=[pl.BlockSpec(memory_space=pltpu.HBM)] * 4,
        out_specs=pl.BlockSpec(memory_space=pltpu.VMEM),
        scratch_shapes=[
            block(nf, rows, polar, LANES),
            block(nf * n, polar, LANES),
            block(n, polar, LANES),
            block(nf * n, polar, LANES),
            block(nf, rows + 4, polar, LANES),
            pltpu.SMEM(shift.shape, jnp.int32),
            pltpu.SMEM(fraction.shape, jnp.float32),
            block(polar, min(2 * LANES, groups * rows)),
            block(rows + 1, polar, LANES),
            pltpu.SemaphoreType.DMA((nf,)),
            pltpu.SemaphoreType.DMA,
            pltpu.SemaphoreType.DMA((2,)),
            pltpu.SemaphoreType.DMA((nf,)),
            pltpu.SemaphoreType.DMA((nf, rows)),
            pltpu.SemaphoreType.DMA((2,)),
            pltpu.SemaphoreType.DMA((nf, 2)),
            pltpu.SemaphoreType.REGULAR,
            pltpu.SemaphoreType.REGULAR,
            pltpu.SemaphoreType.DMA((2,)),
        ],
        compiler_params=pltpu.CompilerParams(
            collective_id=0, has_side_effects=True, vmem_limit_bytes=VMEM_BYTES
        ),
        name="orbital",
    )(shift, fraction, fields, radial_rate.T)


def solution(mesh):
    placed = (P(None, "rad", None, "az"), P(), P(), P())
    body = functools.partial(shards, mesh.shape["az"], mesh.shape["rad"])
    return jax.shard_map(
        body, mesh=mesh, in_specs=placed, out_specs=P(None, "rad", None, "az"), check_vma=False
    )
```
